32 devices in a mesh: section: 4 (over z), tensor: 4 (over y, x), dp: 2 (over core).
Axes of the slice: x: 2, y: 2, z: 4, core: 2. Of those that a mesh axis runs over, the one named last changes fastest.
Arguments:
- forward_rows: bfloat16 [4, 2, 192, 8192], P('section', 'dp', None, 'tensor'), may hold values from -6 to 6
- saved_rows: bfloat16 [4, 2, 192, 8192], P('section', 'dp', None, 'tensor'), may hold values from -40.5 to 40.5
- output_grad: bfloat16 [4, 2, 192, 8192], P('section', 'dp', None, 'tensor'), may hold values from -1.27 to 1.27
- lengths: int32 [4, 2, 2], P('section', 'dp'), may hold values from 1 to 96
- norm_gain: bfloat16 [4, 8192], P('section', 'tensor'), may hold values from 0.5 to 1.5
- down_map: bfloat16 [4, 192, 8192], P('section', None, 'tensor'), may hold values from -0.067396115 to 0.067396115
- up_map: bfloat16 [4, 192, 8192], P('section', None, 'tensor'), may hold values from -1.0625 to 1.0625
Outputs:
- next_inputs: bfloat16 [4, 2, 192, 8192], P('section', 'dp', None, 'tensor')
- next_grads: bfloat16 [4, 2, 192, 8192], P('section', 'dp', None, 'tensor')
- grad_down: bfloat16 [4, 192, 8192], P('section', 'dp', 'tensor')
- grad_up: bfloat16 [4, 192, 8192], P('section', 'dp', 'tensor')
The draws below stay inside these ranges and needn't reach their ends.
All inputs are finite; a program needn't handle non-finite values.
Results may differ from the reference program's by a relative error of at most 0.02.
Values may be sent and summed in bfloat16 or wider, within the bound.
No kernel may reach another device: no remote copies, remote signals or barrier semaphores. Data moves between devices by JAX's collectives and lax.ppermute only.
A program may use at most 64 MiB of HBM per device.

```python
import jax
import jax.numpy as jnp
from jax import lax

D = 8192
R = 192
ROWS = 192
SEQ = 96
N_SECTION = 4
N_DP = 2


def shared_rows(key):
    base = jax.random.fold_in(key, 11)
    shape = (N_SECTION, N_DP, ROWS, D)
    return jnp.clip(jax.random.normal(base, shape, jnp.float32), -6.0, 6.0)


def draw_saved_rows(key, part):
    values = shared_rows(key)
    return values.astype(jnp.bfloat16)


def draw_output_grad(key, part):
    shared = shared_rows(key)
    noise = jax.random.normal(jax.random.fold_in(key, 13), shared.shape, jnp.float32)
    mixed = 0.8 * shared + 0.6 * jnp.clip(noise, -6.0, 6.0)
    return (0.15 * mixed).astype(jnp.bfloat16)


def map_values(key, salt):
    base = jax.random.fold_in(key, salt)
    shape = (N_SECTION, R, D)
    return jnp.clip(jax.random.normal(base, shape, jnp.float32), -6.0, 6.0)


def draw_down_map(key, part):
    return (map_values(key, 21) * D ** (-0.5)).astype(jnp.bfloat16)


def draw_up_map(key, part):
    shared = map_values(key, 21)
    own_part = map_values(key, 22)
    mixed = 0.8 * shared + 0.6 * own_part
    return (mixed * (R // 3) ** (-0.5)).astype(jnp.bfloat16)


def place_ends(result, key, smallest, top_value):
    extent = result.shape
    place = [jax.random.randint(jax.random.fold_in(key, axis), (), 0, extent[axis]) for axis in range(len(extent))]
    result = result.at[tuple(place)].set(smallest)
    longest = extent.index(max(extent))
    place[longest] = (place[longest] + 1) % extent[longest]
    return result.at[tuple(place)].set(top_value)


def level_of(rng, extent, split, smallest, high):
    gain, own = 1.0, jax.random.fold_in(rng, 6)
    for dim, parts in split:
        draws = jnp.exp(jax.random.uniform(jax.random.fold_in(own, dim), (parts,), jnp.float32, smallest / len(split), high / len(split)))
        gain = gain * jnp.repeat(draws, extent[dim] // parts).reshape([-1 if axis == dim else 1 for axis in range(len(extent))])
    return gain


def normal_values(stream_key, dims, scale, most, pieces=(), held_as=jnp.bfloat16):
    factor_of = level_of(stream_key, dims, pieces, -0.22, 0.18) if pieces else 1.0
    values = jax.random.normal(stream_key, dims, jnp.float32) * scale * factor_of
    return jnp.minimum(jnp.maximum(values, -most), most).astype(held_as)


def setup_inputs(seed: int = 0) -> dict:
    seeds = jax.random.split(jax.random.key(seed), 8)
    forward_rows = normal_values(seeds[0], (N_SECTION, N_DP, ROWS, D), 1.0, 6.0, ((0, 4), (1, 2), (3, 4)))
    saved_rows = draw_saved_rows(jax.random.fold_in(seeds[7], 71), 0)
    output_grad = draw_output_grad(jax.random.fold_in(seeds[7], 71), 0)
    lengths = place_ends(jax.random.randint(seeds[3], (N_SECTION, N_DP, 2), 1, SEQ + 1), jax.random.fold_in(seeds[3], 1), 1, SEQ).astype(jnp.int32)
    norm_gain = jnp.clip(1.0 + 0.1 * jax.random.normal(seeds[4], (N_SECTION, D), jnp.float32), 0.5, 1.5).astype(jnp.bfloat16)
    down_map = draw_down_map(jax.random.fold_in(seeds[7], 71), 0)
    up_map = draw_up_map(jax.random.fold_in(seeds[7], 71), 0)
    return dict(forward_rows=forward_rows, saved_rows=saved_rows, output_grad=output_grad, lengths=lengths, norm_gain=norm_gain, down_map=down_map, up_map=up_map)


EPSILON = 1e-05

def contract_last(left_side, right_side):
    return lax.dot_general(left_side, right_side, (((1,), (1,)), ((), ())), preferred_element_type=jnp.float32)

def contract_rows(left_side, right_side):
    return lax.dot_general(left_side, right_side, (((0,), (0,)), ((), ())), preferred_element_type=jnp.float32)

def silu_slope(values):
    gate_value = jax.nn.sigmoid(values)
    return gate_value * (1.0 + values * (1.0 - gate_value))

def norm_rows(row_block, gain_cols):
    values = row_block.astype(jnp.float32)
    scale = lax.rsqrt(lax.optimization_barrier(jnp.mean(values * values, axis=1, keepdims=True)) + EPSILON)
    return (values, scale, (values * scale * gain_cols).astype(jnp.bfloat16))

def group_tick(forward_block, saved_block, incoming, seq_lengths, gain_cols, down_rows, up_rows):
    forward_values, forward_scale, forward_normed = norm_rows(forward_block, gain_cols)
    forward_act = jax.nn.silu(contract_last(forward_normed, down_rows)).astype(jnp.bfloat16)
    forward_out = (forward_values + jnp.dot(forward_act, up_rows, preferred_element_type=jnp.float32)).astype(jnp.bfloat16)
    position = jnp.arange(ROWS, dtype=jnp.int32)
    length_limit = jnp.where(position // SEQ == 0, seq_lengths[0], seq_lengths[1])
    keep_rows = position % SEQ < length_limit
    kept_grad = jnp.where(keep_rows[:, None], incoming, jnp.zeros_like(incoming))
    saved_values, saved_scale, saved_normed = norm_rows(saved_block, gain_cols)
    saved_rank = contract_last(saved_normed, down_rows)
    saved_act = jax.nn.silu(saved_rank).astype(jnp.bfloat16)
    rank_slope = contract_last(kept_grad, up_rows)
    back_rank = (rank_slope * silu_slope(saved_rank)).astype(jnp.bfloat16)
    back_normed = jnp.dot(back_rank, down_rows, preferred_element_type=jnp.float32)
    weighted = gain_cols * back_normed
    correction = lax.optimization_barrier(jnp.mean(saved_values * weighted, axis=1, keepdims=True))
    scale_cube = saved_scale * saved_scale * saved_scale
    grad_rows = (kept_grad.astype(jnp.float32) + saved_scale * weighted - saved_values * scale_cube * correction).astype(jnp.bfloat16)
    down_part = contract_rows(back_rank, saved_normed).astype(jnp.bfloat16)
    up_part = contract_rows(saved_act, kept_grad).astype(jnp.bfloat16)
    return (forward_out, grad_rows, down_part, up_part)

def section_tick(packed):
    forward_block, saved_block, incoming, seq_lengths, gain_row, down_rows, up_rows = packed
    gain_cols = gain_row.astype(jnp.float32)
    group_map = jax.vmap(group_tick, in_axes=(0, 0, 0, 0, None, None, None))
    forward_out, grad_rows, down_part, up_part = group_map(forward_block, saved_block, incoming, seq_lengths, gain_cols, down_rows, up_rows)
    down_part = lax.optimization_barrier(down_part)
    up_part = lax.optimization_barrier(up_part)
    mean_weight = 1.0 / N_DP
    grad_down = (lax.optimization_barrier(jnp.sum(down_part.astype(jnp.float32), axis=0)) * mean_weight).astype(jnp.bfloat16)
    grad_up = (lax.optimization_barrier(jnp.sum(up_part.astype(jnp.float32), axis=0)) * mean_weight).astype(jnp.bfloat16)
    return (forward_out, grad_rows, grad_down, grad_up)

def reference(forward_rows, saved_rows, output_grad, lengths, norm_gain, down_map, up_map):
    forward_out, grad_rows, grad_down, grad_up = lax.map(section_tick, (forward_rows, saved_rows, output_grad, lengths, norm_gain, down_map, up_map))
    next_inputs = jnp.concatenate([jnp.zeros_like(forward_out[:1]), forward_out[:-1]], axis=0)
    next_grads = jnp.concatenate([grad_rows[1:], jnp.zeros_like(grad_rows[:1])], axis=0)
    return (next_inputs, next_grads, grad_down, grad_up)
```

```python
import functools

import jax
import jax.numpy as jnp
from jax import lax
from jax.experimental import pallas as pl
from jax.experimental.pallas import tpu as pltpu
from jax.sharding import PartitionSpec as P

EPSILON = 1e-05
LANES = 128
F32 = jnp.float32
BF16 = jnp.bfloat16


def round_up(value, unit):
    return -(-value // unit) * unit


def partner(index, step, count):
    if count & (count - 1) == 0:
        return index ^ step
    return (index + step) % count


def source(index, step, count):
    if count & (count - 1) == 0:
        return index ^ step
    return (index - step + count) % count


def send_step(cells, axis, step):
    count = lax.axis_size(axis)
    return lax.ppermute(cells, axis, [(i, partner(i, step, count)) for i in range(count)])


def contract_last(left_side, right_side):
    return lax.dot_general(left_side, right_side, (((1,), (1,)), ((), ())), preferred_element_type=F32)


def contract_rows(left_side, right_side):
    return lax.dot_general(left_side, right_side, (((0,), (0,)), ((), ())), preferred_element_type=F32)


def split_pair(values):
    high = values.astype(BF16).astype(F32)
    return high, values - high


def place_pair(slot, unit_count, pair):
    lane = lax.broadcasted_iota(jnp.int32, slot.shape, 1)
    high, low = pair
    rest = jnp.where(lane == unit_count, high, jnp.where(lane == unit_count + 1, low, 0.0))
    return jnp.where(lane < unit_count, slot, rest)


def take_pair(slot, unit_count):
    return slot[:, unit_count : unit_count + 1] + slot[:, unit_count + 1 : unit_count + 2]


def keep_mask(first_row, shape, seq_rows, lengths_ref):
    row = first_row + lax.broadcasted_iota(jnp.int32, shape, 0)
    limit = jnp.where(row < seq_rows, lengths_ref[0], lengths_ref[1] + seq_rows)
    return row < limit


def partials_body(unit_count, slot, share_count, place_ref, fwd_ref, saved_ref, grad_ref, gain_ref, down_ref, up_ref, *refs):
    outs = refs[:share_count]
    acc_ref, squares_ref = refs[share_count:]
    step = pl.program_id(0)

    @pl.when(step == 0)
    def _():
        acc_ref[...] = jnp.zeros_like(acc_ref)
        squares_ref[...] = jnp.zeros_like(squares_ref)

    gain = gain_ref[...].astype(F32)
    down = down_ref[...]
    for which, rows_ref in enumerate((fwd_ref, saved_ref)):
        values = rows_ref[...].astype(F32)
        lo = which * slot
        acc_ref[:, lo : lo + unit_count] += contract_last((values * gain).astype(BF16), down)
        total = squares_ref[which]
        for c in range(0, values.shape[1], LANES):
            part = values[:, c : c + LANES]
            total += part * part
        squares_ref[which] = total
    acc_ref[:, 2 * slot : 2 * slot + unit_count] += contract_last(grad_ref[...], up_ref[...])

    @pl.when(step == pl.num_programs(0) - 1)
    def _():
        for which in range(2):
            total = jnp.sum(squares_ref[which], axis=1, keepdims=True)
            lo = which * slot
            acc_ref[:, lo : lo + slot] = place_pair(acc_ref[:, lo : lo + slot], unit_count, split_pair(total))
        share_rows = outs[0].shape[0]
        for k, out in enumerate(outs):
            first = pl.multiple_of(partner(place_ref[0], k, share_count) * share_rows, share_rows)
            out[...] = acc_ref[pl.ds(first, share_rows), :].astype(BF16)


def middle_body(unit_count, slot, full_width, seq_rows, place_ref, lengths_ref, *refs):
    parts, out = refs[:-1], refs[-1]
    total = parts[0][...].astype(F32)
    for part in parts[1:]:
        total += part[...].astype(F32)
    share_rows = total.shape[0]
    keep = keep_mask(place_ref[0] * share_rows, (share_rows, slot), seq_rows, lengths_ref)
    fwd, saved, slope = (total[:, i * slot : (i + 1) * slot] for i in range(3))
    fwd_scale = lax.rsqrt(take_pair(fwd, unit_count) / full_width + EPSILON)
    saved_scale = lax.rsqrt(take_pair(saved, unit_count) / full_width + EPSILON)
    lane = lax.broadcasted_iota(jnp.int32, fwd.shape, 1)
    unit = lane < unit_count
    fwd_rank = fwd * fwd_scale
    saved_rank = saved * saved_scale
    gate = jax.nn.sigmoid(saved_rank)
    back = jnp.where(unit & keep, slope * (gate * (1.0 + saved_rank * (1.0 - gate))), 0.0)
    bend = saved_scale * saved_scale * (jnp.sum(back * saved_rank, axis=1, keepdims=True) / full_width)
    out[:, 0:slot] = jnp.where(unit, fwd_rank * jax.nn.sigmoid(fwd_rank), 0.0).astype(BF16)
    out[:, slot : 2 * slot] = jnp.where(unit & keep, saved_rank * gate, 0.0).astype(BF16)
    out[:, 2 * slot :] = place_pair(back * saved_scale, unit_count, split_pair(bend)).astype(BF16)


def join_shares(place_ref, shares, whole_ref):
    share_rows = shares[0].shape[0]
    for k, share in enumerate(shares):
        first = source(place_ref[0], k, len(shares)) * share_rows
        whole_ref[pl.ds(pl.multiple_of(first, share_rows), share_rows), :] = share[...]


def edges_body(unit_count, slot, share_count, seq_rows, place_ref, lengths_ref, *refs):
    shares = refs[:share_count]
    fwd_ref, saved_ref, grad_ref, gain_ref, down_ref, up_ref, out_fwd, out_grad, whole_ref = refs[share_count:]

    @pl.when(pl.program_id(0) == 0)
    def _():
        join_shares(place_ref, shares, whole_ref)

    keep = keep_mask(0, grad_ref.shape, seq_rows, lengths_ref)
    back = whole_ref[:, 2 * slot : 2 * slot + unit_count]
    bend = take_pair(whole_ref[:, 2 * slot :].astype(F32), unit_count)
    weighted = jnp.dot(back, down_ref[...], preferred_element_type=F32) * gain_ref[...].astype(F32)
    kept = jnp.where(keep, grad_ref[...].astype(F32), 0.0)
    out_grad[...] = (kept + weighted - saved_ref[...].astype(F32) * bend).astype(BF16)
    act = whole_ref[:, 0:unit_count]
    lifted = jnp.dot(act, up_ref[...], preferred_element_type=F32)
    out_fwd[...] = (fwd_ref[...].astype(F32) + lifted).astype(BF16)


def grads_body(unit_count, slot, share_count, place_ref, *refs):
    shares = refs[:share_count]
    saved_ref, grad_ref, gain_ref = refs[share_count : share_count + 3]
    outs = refs[share_count + 3 : -2]
    whole_ref, hold_ref = refs[-2:]

    @pl.when(pl.program_id(0) == 0)
    def _():
        join_shares(place_ref, shares, whole_ref)

    back = whole_ref[:, 2 * slot : 2 * slot + unit_count]
    act = whole_ref[:, slot : slot + unit_count]
    hold_ref[0] = contract_rows(back, saved_ref[...]) * gain_ref[...].astype(F32)
    hold_ref[1] = contract_rows(act, grad_ref[...])
    group_count = len(outs)
    group_rows = unit_count // group_count
    for k, out in enumerate(outs):
        first = partner(place_ref[1], k, group_count) * group_rows
        for which in range(2):
            out[which] = hold_ref[which, pl.ds(pl.multiple_of(first, group_rows), group_rows), :].astype(BF16)


def shards(forward_rows, saved_rows, output_grad, lengths, norm_gain, down_map, up_map):
    fwd, saved, grad = forward_rows[0, 0], saved_rows[0, 0], output_grad[0, 0]
    seq_lengths = lengths[0, 0]
    down, up = down_map[0], up_map[0]
    row_count, width = fwd.shape
    unit_count = down.shape[0]
    share_count = lax.axis_size("tensor")
    group_count = lax.axis_size("dp")
    section_count = lax.axis_size("section")
    share_rows = row_count // share_count
    seq_rows = row_count // 2
    full_width = width * share_count
    slot = round_up(unit_count + 2, LANES)
    packed = 3 * slot
    place = jnp.stack([lax.axis_index("tensor"), lax.axis_index("dp")]).astype(jnp.int32)
    block = min(width, 512)
    steps = width // block
    smem = pl.BlockSpec(memory_space=pltpu.SMEM)
    cols = lambda n: pl.BlockSpec((n, block), lambda j: (0, j))
    whole = pl.BlockSpec((share_rows, packed), lambda j: (0, 0))
    share_type = jax.ShapeDtypeStruct((share_rows, packed), BF16)

    parts = pl.pallas_call(
        functools.partial(partials_body, unit_count, slot, share_count),
        grid=(steps,),
        in_specs=[smem, cols(row_count), cols(row_count), cols(row_count), cols(1), cols(unit_count), cols(unit_count)],
        out_specs=[whole] * share_count,
        out_shape=[share_type] * share_count,
        scratch_shapes=[pltpu.VMEM((row_count, packed), F32), pltpu.VMEM((2, row_count, LANES), F32)],
        name="partials",
    )(place, fwd, saved, grad, norm_gain, down, up)
    got = [parts[0]] + [send_step(parts[k], "tensor", k) for k in range(1, share_count)]
    mine = pl.pallas_call(
        functools.partial(middle_body, unit_count, slot, full_width, seq_rows),
        in_specs=[smem, smem] + [pl.BlockSpec(memory_space=pltpu.VMEM)] * share_count,
        out_specs=pl.BlockSpec(memory_space=pltpu.VMEM),
        out_shape=share_type,
        name="middle",
    )(place, seq_lengths, *got)
    shares = [mine] + [send_step(mine, "tensor", k) for k in range(1, share_count)]
    out_fwd, out_grad = pl.pallas_call(
        functools.partial(edges_body, unit_count, slot, share_count, seq_rows),
        grid=(steps,),
        in_specs=[smem, smem] + [whole] * share_count
        + [cols(row_count), cols(row_count), cols(row_count), cols(1), cols(unit_count), cols(unit_count)],
        out_specs=[cols(row_count)] * 2,
        out_shape=[jax.ShapeDtypeStruct((row_count, width), BF16)] * 2,
        scratch_shapes=[pltpu.VMEM((row_count, packed), BF16)],
        name="edges",
    )(place, seq_lengths, *shares, fwd, saved, grad, norm_gain, down, up)
    next_grads = lax.ppermute(out_grad, "section", [(i + 1, i) for i in range(section_count - 1)])
    next_inputs = lax.ppermute(out_fwd, "section", [(i, i + 1) for i in range(section_count - 1)])
    group_rows = unit_count // group_count
    halves = pl.pallas_call(
        functools.partial(grads_body, unit_count, slot, share_count),
        grid=(steps,),
        in_specs=[smem] + [whole] * share_count + [cols(row_count), cols(row_count), cols(1)],
        out_specs=[pl.BlockSpec((2, group_rows, block), lambda j: (0, 0, j))] * group_count,
        out_shape=[jax.ShapeDtypeStruct((2, group_rows, width), BF16)] * group_count,
        scratch_shapes=[pltpu.VMEM((row_count, packed), BF16), pltpu.VMEM((2, unit_count, block), F32)],
        name="grads",
    )(place, *shares, saved, grad, norm_gain)
    total = halves[0].astype(F32)
    for k in range(1, group_count):
        total += send_step(halves[k], "dp", k).astype(F32)
    mean = (total * (1.0 / group_count)).astype(BF16)
    return (next_inputs[None, None], next_grads[None, None], mean[0:1], mean[1:2])


def solution(mesh):
    rows = P("section", "dp", None, "tensor")
    maps = P("section", None, "tensor")
    return jax.shard_map(
        shards,
        mesh=mesh,
        in_specs=(rows, rows, rows, P("section", "dp", None), P("section", "tensor"), maps, maps),
        out_specs=(rows, rows, P("section", "dp", "tensor"), P("section", "dp", "tensor")),
        check_vma=False,
    )
```

```python
import functools

import jax
import jax.numpy as jnp
from jax import lax
from jax.experimental import pallas as pl
from jax.experimental.pallas import tpu as pltpu
from jax.sharding import PartitionSpec as P

EPSILON = 1e-05
LANES = 128
BLOCK = 512
F32 = jnp.float32
BF16 = jnp.bfloat16


def round_up(value, unit):
    return -(-value // unit) * unit


def partner(index, step, count):
    if count & (count - 1) == 0:
        return index ^ step
    return (index + step) % count


def source(index, step, count):
    if count & (count - 1) == 0:
        return index ^ step
    return (index - step + count) % count


def send_step(cells, axis, step):
    count = lax.axis_size(axis)
    return lax.ppermute(cells, axis, [(i, partner(i, step, count)) for i in range(count)])


def near(cells):
    return pltpu.with_memory_space_constraint(cells, pltpu.VMEM)


def contract_last(left_side, right_side):
    return lax.dot_general(left_side, right_side, (((1,), (1,)), ((), ())), preferred_element_type=F32)


def contract_rows(left_side, right_side):
    return lax.dot_general(left_side, right_side, (((0,), (0,)), ((), ())), preferred_element_type=F32)


def split_pair(values):
    high = values.astype(BF16).astype(F32)
    return high, values - high


def place_pair(slot, unit_count, pair):
    lane = lax.broadcasted_iota(jnp.int32, slot.shape, 1)
    high, low = pair
    rest = jnp.where(lane == unit_count, high, jnp.where(lane == unit_count + 1, low, 0.0))
    return jnp.where(lane < unit_count, slot, rest)


def take_pair(slot, unit_count):
    return slot[:, unit_count : unit_count + 1] + slot[:, unit_count + 1 : unit_count + 2]


def keep_mask(first_row, shape, seq_rows, lengths_ref):
    row = first_row + lax.broadcasted_iota(jnp.int32, shape, 0)
    limit = jnp.where(row < seq_rows, lengths_ref[0], lengths_ref[1] + seq_rows)
    return row < limit


def partials_body(unit_count, slot, share_count, fwd_ref, saved_ref, grad_ref, gain_ref, down_ref, up_ref, *refs):
    outs = refs[:share_count]
    acc_ref, squares_ref = refs[share_count:]
    step = pl.program_id(0)

    @pl.when(step == 0)
    def _():
        acc_ref[...] = jnp.zeros_like(acc_ref)
        squares_ref[...] = jnp.zeros_like(squares_ref)

    gain = gain_ref[...].astype(F32)
    down = down_ref[...]
    for which, rows_ref in enumerate((fwd_ref, saved_ref)):
        values = rows_ref[...].astype(F32)
        lo = which * slot
        acc_ref[:, lo : lo + unit_count] += contract_last((values * gain).astype(BF16), down)
        total = squares_ref[which]
        for c in range(0, values.shape[1], LANES):
            part = values[:, c : c + LANES]
            total += part * part
        squares_ref[which] = total
    acc_ref[:, 2 * slot : 2 * slot + unit_count] += contract_last(grad_ref[...], up_ref[...])

    @pl.when(step == pl.num_programs(0) - 1)
    def _():
        for which in range(2):
            total = jnp.sum(squares_ref[which], axis=1, keepdims=True)
            lo = which * slot
            acc_ref[:, lo : lo + slot] = place_pair(acc_ref[:, lo : lo + slot], unit_count, split_pair(total))
        share_rows = outs[0].shape[0]
        for k, out in enumerate(outs):
            first = pl.multiple_of(partner(lax.axis_index("tensor"), k, share_count) * share_rows, share_rows)
            out[...] = acc_ref[pl.ds(first, share_rows), :].astype(BF16)


def middle_body(unit_count, slot, full_width, seq_rows, lengths_ref, *refs):
    parts, out = refs[:-1], refs[-1]
    total = parts[0][...].astype(F32)
    for part in parts[1:]:
        total += part[...].astype(F32)
    share_rows = total.shape[0]
    keep = keep_mask(lax.axis_index("tensor") * share_rows, (share_rows, slot), seq_rows, lengths_ref)
    fwd, saved, slope = (total[:, i * slot : (i + 1) * slot] for i in range(3))
    fwd_scale = lax.rsqrt(take_pair(fwd, unit_count) / full_width + EPSILON)
    saved_scale = lax.rsqrt(take_pair(saved, unit_count) / full_width + EPSILON)
    lane = lax.broadcasted_iota(jnp.int32, fwd.shape, 1)
    unit = lane < unit_count
    fwd_rank = fwd * fwd_scale
    saved_rank = saved * saved_scale
    gate = jax.nn.sigmoid(saved_rank)
    back = jnp.where(unit & keep, slope * (gate * (1.0 + saved_rank * (1.0 - gate))), 0.0)
    bend = saved_scale * saved_scale * (jnp.sum(back * saved_rank, axis=1, keepdims=True) / full_width)
    out[:, 0:slot] = jnp.where(unit, fwd_rank * jax.nn.sigmoid(fwd_rank), 0.0).astype(BF16)
    out[:, slot : 2 * slot] = jnp.where(unit & keep, saved_rank * gate, 0.0).astype(BF16)
    out[:, 2 * slot :] = place_pair(back * saved_scale, unit_count, split_pair(bend)).astype(BF16)


def join_shares(shares, whole_ref):
    share_rows = shares[0].shape[0]
    for k, share in enumerate(shares):
        first = source(lax.axis_index("tensor"), k, len(shares)) * share_rows
        whole_ref[pl.ds(pl.multiple_of(first, share_rows), share_rows), :] = share[...]


def edges_body(unit_count, slot, share_count, seq_rows, lengths_ref, *refs):
    shares = refs[:share_count]
    fwd_ref, saved_ref, grad_ref, gain_ref, down_ref, up_ref, out_fwd, out_grad, whole_ref = refs[share_count:]

    @pl.when(pl.program_id(0) == 0)
    def _():
        join_shares(shares, whole_ref)

    block = grad_ref.shape[1]
    here = pl.ds(pl.multiple_of(pl.program_id(0) * block, block), block)
    keep = keep_mask(0, grad_ref.shape, seq_rows, lengths_ref)
    back = whole_ref[:, 2 * slot : 2 * slot + unit_count]
    bend = take_pair(whole_ref[:, 2 * slot :].astype(F32), unit_count)
    weighted = jnp.dot(back, down_ref[...], preferred_element_type=F32) * gain_ref[...].astype(F32)
    kept = jnp.where(keep, grad_ref[...].astype(F32), 0.0)
    out_grad[:, here] = (kept + weighted - saved_ref[...].astype(F32) * bend).astype(BF16)
    act = whole_ref[:, 0:unit_count]
    lifted = jnp.dot(act, up_ref[...], preferred_element_type=F32)
    out_fwd[:, here] = (fwd_ref[...].astype(F32) + lifted).astype(BF16)


def grads_body(unit_count, slot, share_count, *refs):
    shares = refs[:share_count]
    saved_ref, grad_ref, gain_ref = refs[share_count : share_count + 3]
    outs = refs[share_count + 3 : -2]
    whole_ref, hold_ref = refs[-2:]

    @pl.when(pl.program_id(0) == 0)
    def _():
        join_shares(shares, whole_ref)

    back = whole_ref[:, 2 * slot : 2 * slot + unit_count]
    act = whole_ref[:, slot : slot + unit_count]
    hold_ref[0] = contract_rows(back, saved_ref[...]) * gain_ref[...].astype(F32)
    hold_ref[1] = contract_rows(act, grad_ref[...])
    group_count = len(outs)
    group_rows = unit_count // group_count
    for k, out in enumerate(outs):
        first = partner(lax.axis_index("dp"), k, group_count) * group_rows
        for which in range(2):
            out[which] = hold_ref[which, pl.ds(pl.multiple_of(first, group_rows), group_rows), :].astype(BF16)


def land_body(first_ref, second_ref, first_out, second_out, first_sem, second_sem):
    first = pltpu.make_async_copy(first_ref, first_out, first_sem)
    second = pltpu.make_async_copy(second_ref, second_out, second_sem)
    first.start()
    second.start()
    first.wait()
    second.wait()


def shards(forward_rows, saved_rows, output_grad, lengths, norm_gain, down_map, up_map):
    fwd, saved, grad = forward_rows[0, 0], saved_rows[0, 0], output_grad[0, 0]
    seq_lengths = lengths[0, 0]
    down, up = down_map[0], up_map[0]
    row_count, width = fwd.shape
    unit_count = down.shape[0]
    share_count = lax.axis_size("tensor")
    group_count = lax.axis_size("dp")
    section_count = lax.axis_size("section")
    share_rows = row_count // share_count
    seq_rows = row_count // 2
    full_width = width * share_count
    slot = round_up(unit_count + 2, LANES)
    packed = 3 * slot
    block = min(width, BLOCK)
    steps = width // block
    smem = pl.BlockSpec(memory_space=pltpu.SMEM)
    cols = lambda n: pl.BlockSpec((n, block), lambda j: (0, j))
    whole = pl.BlockSpec(memory_space=pltpu.VMEM)
    share_type = pltpu.VMEM((share_rows, packed), BF16)

    parts = pl.pallas_call(
        functools.partial(partials_body, unit_count, slot, share_count),
        grid=(steps,),
        in_specs=[cols(row_count), cols(row_count), cols(row_count), cols(1), cols(unit_count), cols(unit_count)],
        out_specs=[whole] * share_count,
        out_shape=[share_type] * share_count,
        scratch_shapes=[pltpu.VMEM((row_count, packed), F32), pltpu.VMEM((2, row_count, LANES), F32)],
        name="partials",
    )(fwd, saved, grad, norm_gain, down, up)
    got = [near(parts[0])] + [near(send_step(parts[k], "tensor", k)) for k in range(1, share_count)]
    mine = pl.pallas_call(
        functools.partial(middle_body, unit_count, slot, full_width, seq_rows),
        in_specs=[smem] + [pl.BlockSpec(memory_space=pltpu.VMEM)] * share_count,
        out_specs=pl.BlockSpec(memory_space=pltpu.VMEM),
        out_shape=share_type,
        name="middle",
    )(seq_lengths, *got)
    shares = [near(mine)] + [near(send_step(mine, "tensor", k)) for k in range(1, share_count)]
    out_fwd, out_grad = pl.pallas_call(
        functools.partial(edges_body, unit_count, slot, share_count, seq_rows),
        grid=(steps,),
        in_specs=[smem] + [whole] * share_count
        + [cols(row_count), cols(row_count), cols(row_count), cols(1), cols(unit_count), cols(unit_count)],
        out_specs=[whole] * 2,
        out_shape=[pltpu.VMEM((row_count, width), BF16)] * 2,
        scratch_shapes=[pltpu.VMEM((row_count, packed), BF16)],
        name="edges",
    )(seq_lengths, *shares, fwd, saved, grad, norm_gain, down, up)
    next_grads = lax.ppermute(near(out_grad), "section", [(i + 1, i) for i in range(section_count - 1)])
    next_inputs = lax.ppermute(near(out_fwd), "section", [(i, i + 1) for i in range(section_count - 1)])
    group_rows = unit_count // group_count
    sum_maps = pl.pallas_call(
        functools.partial(grads_body, unit_count, slot, share_count),
        grid=(steps,),
        in_specs=[whole] * share_count + [cols(row_count), cols(row_count), cols(1)],
        out_specs=[pl.BlockSpec((2, group_rows, block), lambda j: (0, 0, j))] * group_count,
        out_shape=[jax.ShapeDtypeStruct((2, group_rows, width), BF16)] * group_count,
        scratch_shapes=[pltpu.VMEM((row_count, packed), BF16), pltpu.VMEM((2, unit_count, block), F32)],
        cost_estimate=pl.CostEstimate(flops=40 * row_count * unit_count * width, bytes_accessed=6 * row_count * width, transcendentals=0),
        name="grads",
    )
    halves = sum_maps(*shares, saved, grad, norm_gain)
    total = halves[0].astype(F32)
    for k in range(1, group_count):
        total += send_step(halves[k], "dp", k).astype(F32)
    mean = (total * (1.0 / group_count)).astype(BF16)
    next_inputs, next_grads = pl.pallas_call(
        land_body,
        in_specs=[whole] * 2,
        out_specs=[pl.BlockSpec(memory_space=pl.ANY)] * 2,
        out_shape=[jax.ShapeDtypeStruct((row_count, width), BF16)] * 2,
        scratch_shapes=[pltpu.SemaphoreType.DMA] * 2,
        name="land",
    )(near(next_inputs), near(next_grads))
    return (next_inputs[None, None], next_grads[None, None], mean[0:1], mean[1:2])


def solution(mesh):
    rows = P("section", "dp", None, "tensor")
    maps = P("section", None, "tensor")
    return jax.shard_map(
        shards,
        mesh=mesh,
        in_specs=(rows, rows, rows, P("section", "dp", None), P("section", "tensor"), maps, maps),
        out_specs=(rows, rows, P("section", "dp", "tensor"), P("section", "dp", "tensor")),
        check_vma=False,
    )
```

```python
import functools

import jax
import jax.numpy as jnp
from jax import lax
from jax.experimental import pallas as pl
from jax.experimental.pallas import tpu as pltpu
from jax.sharding import PartitionSpec as P

EPSILON = 1e-05
LANES = 128
BLOCK = 512
CHUNKS = 2
F32 = jnp.float32
BF16 = jnp.bfloat16


def round_up(value, unit):
    return -(-value // unit) * unit


def partner(index, step, count):
    if count & (count - 1) == 0:
        return index ^ step
    return (index + step) % count


def source(index, step, count):
    if count & (count - 1) == 0:
        return index ^ step
    return (index - step + count) % count


def send_step(cells, axis, step):
    count = lax.axis_size(axis)
    return lax.ppermute(cells, axis, [(i, partner(i, step, count)) for i in range(count)])


def near(cells):
    return pltpu.with_memory_space_constraint(cells, pltpu.VMEM)


def contract_last(left_side, right_side):
    return lax.dot_general(left_side, right_side, (((1,), (1,)), ((), ())), preferred_element_type=F32)


def contract_rows(left_side, right_side):
    return lax.dot_general(left_side, right_side, (((0,), (0,)), ((), ())), preferred_element_type=F32)


def split_pair(values):
    high = values.astype(BF16).astype(F32)
    return high, values - high


def place_pair(slot, unit_count, pair):
    lane = lax.broadcasted_iota(jnp.int32, slot.shape, 1)
    high, low = pair
    rest = jnp.where(lane == unit_count, high, jnp.where(lane == unit_count + 1, low, 0.0))
    return jnp.where(lane < unit_count, slot, rest)


def take_pair(slot, unit_count):
    return slot[:, unit_count : unit_count + 1] + slot[:, unit_count + 1 : unit_count + 2]


def keep_mask(first_row, shape, seq_rows, lengths_ref):
    row = first_row + lax.broadcasted_iota(jnp.int32, shape, 0)
    limit = jnp.where(row < seq_rows, lengths_ref[0], lengths_ref[1] + seq_rows)
    return row < limit


def partials_body(unit_count, slot, share_count, fwd_ref, saved_ref, grad_ref, gain_ref, down_ref, up_ref, *refs):
    outs = refs[:share_count]
    acc_ref, squares_ref = refs[share_count:]
    step = pl.program_id(0)

    @pl.when(step == 0)
    def _():
        acc_ref[...] = jnp.zeros_like(acc_ref)
        squares_ref[...] = jnp.zeros_like(squares_ref)

    down = (down_ref[...].astype(F32) * gain_ref[...].astype(F32)).astype(BF16)
    for which, rows_ref in enumerate((fwd_ref, saved_ref)):
        values = rows_ref[...].astype(F32)
        lo = which * slot
        acc_ref[:, lo : lo + unit_count] += contract_last(rows_ref[...], down)
        total = squares_ref[which]
        for c in range(0, values.shape[1], LANES):
            part = values[:, c : c + LANES]
            total += part * part
        squares_ref[which] = total
    acc_ref[:, 2 * slot : 2 * slot + unit_count] += contract_last(grad_ref[...], up_ref[...])

    @pl.when(step == pl.num_programs(0) - 1)
    def _():
        for which in range(2):
            total = jnp.sum(squares_ref[which], axis=1, keepdims=True)
            lo = which * slot
            acc_ref[:, lo : lo + slot] = place_pair(acc_ref[:, lo : lo + slot], unit_count, split_pair(total))
        share_rows = outs[0].shape[0]
        for k, out in enumerate(outs):
            first = pl.multiple_of(partner(lax.axis_index("tensor"), k, share_count) * share_rows, share_rows)
            out[...] = acc_ref[pl.ds(first, share_rows), :].astype(BF16)


def middle_body(unit_count, slot, full_width, seq_rows, lengths_ref, *refs):
    parts, out = refs[:-1], refs[-1]
    total = parts[0][...].astype(F32)
    for part in parts[1:]:
        total += part[...].astype(F32)
    share_rows = total.shape[0]
    keep = keep_mask(lax.axis_index("tensor") * share_rows, (share_rows, slot), seq_rows, lengths_ref)
    fwd, saved, slope = (total[:, i * slot : (i + 1) * slot] for i in range(3))
    fwd_scale = lax.rsqrt(take_pair(fwd, unit_count) / full_width + EPSILON)
    saved_scale = lax.rsqrt(take_pair(saved, unit_count) / full_width + EPSILON)
    lane = lax.broadcasted_iota(jnp.int32, fwd.shape, 1)
    unit = lane < unit_count
    fwd_rank = fwd * fwd_scale
    saved_rank = saved * saved_scale
    gate = jax.nn.sigmoid(saved_rank)
    back = jnp.where(unit & keep, slope * (gate * (1.0 + saved_rank * (1.0 - gate))), 0.0)
    bend = saved_scale * saved_scale * (jnp.sum(back * saved_rank, axis=1, keepdims=True) / full_width)
    out[:, 0:slot] = jnp.where(unit, fwd_rank * jax.nn.sigmoid(fwd_rank), 0.0).astype(BF16)
    out[:, slot : 2 * slot] = jnp.where(unit & keep, saved_rank * gate, 0.0).astype(BF16)
    out[:, 2 * slot :] = place_pair(back * saved_scale, unit_count, split_pair(bend)).astype(BF16)


def join_shares(shares, whole_ref):
    share_rows = shares[0].shape[0]
    for k, share in enumerate(shares):
        first = source(lax.axis_index("tensor"), k, len(shares)) * share_rows
        whole_ref[pl.ds(pl.multiple_of(first, share_rows), share_rows), :] = share[...]


def edges_body(unit_count, slot, share_count, seq_rows, lengths_ref, *refs):
    shares = refs[:share_count]
    fwd_ref, saved_ref, grad_ref, gain_ref, down_ref, up_ref, out_fwd, out_grad, whole_ref = refs[share_count:]

    @pl.when(pl.program_id(0) == 0)
    def _():
        join_shares(shares, whole_ref)

    block = grad_ref.shape[1]
    here = pl.ds(pl.multiple_of(pl.program_id(0) * block, block), block)
    keep = keep_mask(0, grad_ref.shape, seq_rows, lengths_ref)
    back = whole_ref[:, 2 * slot : 2 * slot + unit_count]
    bend = take_pair(whole_ref[:, 2 * slot :].astype(F32), unit_count)
    weighted = jnp.dot(back, down_ref[...], preferred_element_type=F32) * gain_ref[...].astype(F32)
    kept = jnp.where(keep, grad_ref[...].astype(F32), 0.0)
    out_grad[:, here] = (kept + weighted - saved_ref[...].astype(F32) * bend).astype(BF16)
    act = whole_ref[:, 0:unit_count]
    lifted = jnp.dot(act, up_ref[...], preferred_element_type=F32)
    out_fwd[:, here] = (fwd_ref[...].astype(F32) + lifted).astype(BF16)


def grads_body(unit_count, slot, share_count, *refs):
    shares = refs[:share_count]
    saved_ref, grad_ref, gain_ref = refs[share_count : share_count + 3]
    outs = refs[share_count + 3 : -2]
    whole_ref, hold_ref = refs[-2:]

    @pl.when(pl.program_id(0) == 0)
    def _():
        join_shares(shares, whole_ref)

    back = whole_ref[:, 2 * slot : 2 * slot + unit_count]
    act = whole_ref[:, slot : slot + unit_count]
    hold_ref[0] = contract_rows(back, saved_ref[...]) * gain_ref[...].astype(F32)
    hold_ref[1] = contract_rows(act, grad_ref[...])
    group_count = len(outs)
    group_rows = unit_count // group_count
    block = grad_ref.shape[1]
    here = pl.ds(pl.multiple_of(pl.program_id(0) * block, block), block)
    for k, out in enumerate(outs):
        first = partner(lax.axis_index("dp"), k, group_count) * group_rows
        for which in range(2):
            out[which, :, here] = hold_ref[which, pl.ds(pl.multiple_of(first, group_rows), group_rows), :].astype(BF16)


def mean_body(*refs):
    shares, outs = refs[:-2], refs[-2:]
    block = outs[0].shape[1]
    here = pl.ds(pl.multiple_of(pl.program_id(0) * block, block), block)
    for which, out in enumerate(outs):
        total = shares[0][which, :, here].astype(F32)
        for share in shares[1:]:
            total += share[which, :, here].astype(F32)
        out[...] = (total * (1.0 / len(shares))).astype(BF16)


def land_body(first_col, span, first_ref, second_ref, *refs):
    first_out, second_out, first_sem, second_sem = refs[-4:]
    here = pl.ds(first_col, span)
    first = pltpu.make_async_copy(first_ref, first_out.at[:, here], first_sem)
    second = pltpu.make_async_copy(second_ref, second_out.at[:, here], second_sem)
    first.start()
    second.start()
    first.wait()
    second.wait()


def shards(forward_rows, saved_rows, output_grad, lengths, norm_gain, down_map, up_map):
    fwd, saved, grad = forward_rows[0, 0], saved_rows[0, 0], output_grad[0, 0]
    seq_lengths = lengths[0, 0]
    down, up = down_map[0], up_map[0]
    row_count, width = fwd.shape
    unit_count = down.shape[0]
    share_count = lax.axis_size("tensor")
    group_count = lax.axis_size("dp")
    section_count = lax.axis_size("section")
    share_rows = row_count // share_count
    seq_rows = row_count // 2
    full_width = width * share_count
    slot = round_up(unit_count + 2, LANES)
    packed = 3 * slot
    block = min(width, BLOCK)
    steps = width // block
    smem = pl.BlockSpec(memory_space=pltpu.SMEM)
    cols = lambda n: pl.BlockSpec((n, block), lambda j: (0, j))
    whole = pl.BlockSpec(memory_space=pltpu.VMEM)
    share_type = pltpu.VMEM((share_rows, packed), BF16)

    parts = pl.pallas_call(
        functools.partial(partials_body, unit_count, slot, share_count),
        grid=(steps,),
        in_specs=[cols(row_count), cols(row_count), cols(row_count), cols(1), cols(unit_count), cols(unit_count)],
        out_specs=[whole] * share_count,
        out_shape=[share_type] * share_count,
        scratch_shapes=[pltpu.VMEM((row_count, packed), F32), pltpu.VMEM((2, row_count, LANES), F32)],
        name="partials",
    )(fwd, saved, grad, norm_gain, down, up)
    got = [near(send_step(parts[k], "tensor", k)) for k in range(share_count - 1, 0, -1)] + [near(parts[0])]
    mine = pl.pallas_call(
        functools.partial(middle_body, unit_count, slot, full_width, seq_rows),
        in_specs=[smem] + [pl.BlockSpec(memory_space=pltpu.VMEM)] * share_count,
        out_specs=pl.BlockSpec(memory_space=pltpu.VMEM),
        out_shape=share_type,
        name="middle",
    )(seq_lengths, *got)
    shares = [near(mine)] + [near(send_step(mine, "tensor", k)) for k in range(1, share_count)]
    span = width // CHUNKS
    chunk_steps = span // block
    landed = []
    for c in range(CHUNKS):
        part = lambda n, first=c * chunk_steps: pl.BlockSpec((n, block), lambda j: (0, j + first))
        edge_rows = pl.pallas_call(
            functools.partial(edges_body, unit_count, slot, share_count, seq_rows),
            grid=(chunk_steps,),
            in_specs=[smem] + [whole] * share_count
            + [part(row_count), part(row_count), part(row_count), part(1), part(unit_count), part(unit_count)],
            out_specs=[whole] * 2,
            out_shape=[pltpu.VMEM((row_count, span), BF16)] * 2,
            scratch_shapes=[pltpu.VMEM((row_count, packed), BF16)],
            cost_estimate=pl.CostEstimate(flops=40 * row_count * unit_count * span, bytes_accessed=8 * row_count * span, transcendentals=0),
            name="edges",
        )
        out_fwd, out_grad = edge_rows(seq_lengths, *shares, fwd, saved, grad, norm_gain, down, up)
        next_grads = lax.ppermute(near(out_grad), "section", [(i + 1, i) for i in range(section_count - 1)])
        next_inputs = lax.ppermute(near(out_fwd), "section", [(i, i + 1) for i in range(section_count - 1)])
        landed.append((next_inputs, next_grads))
    group_rows = unit_count // group_count
    sum_maps = pl.pallas_call(
        functools.partial(grads_body, unit_count, slot, share_count),
        grid=(steps,),
        in_specs=[whole] * share_count + [cols(row_count), cols(row_count), cols(1)],
        out_specs=[whole] * group_count,
        out_shape=[pltpu.VMEM((2, group_rows, width), BF16)] * group_count,
        scratch_shapes=[pltpu.VMEM((row_count, packed), BF16), pltpu.VMEM((2, unit_count, block), F32)],
        cost_estimate=pl.CostEstimate(flops=40 * row_count * unit_count * width, bytes_accessed=6 * row_count * width, transcendentals=0),
        name="grads",
    )
    halves = sum_maps(*shares, saved, grad, norm_gain)
    sums = [near(halves[0])] + [near(send_step(near(halves[k]), "dp", k)) for k in range(1, group_count)]
    mean_maps = pl.pallas_call(
        mean_body,
        grid=(steps,),
        in_specs=[whole] * group_count,
        out_specs=[cols(group_rows)] * 2,
        out_shape=[jax.ShapeDtypeStruct((group_rows, width), BF16)] * 2,
        name="means",
    )
    grad_down, grad_up = mean_maps(*sums)
    outs = []
    for c, pair in enumerate(landed):
        outs = pl.pallas_call(
            functools.partial(land_body, c * span, span),
            in_specs=[whole] * 2 + [pl.BlockSpec(memory_space=pl.ANY)] * len(outs),
            out_specs=[pl.BlockSpec(memory_space=pl.ANY)] * 2,
            out_shape=[jax.ShapeDtypeStruct((row_count, width), BF16)] * 2,
            input_output_aliases={2: 0, 3: 1} if outs else {},
            scratch_shapes=[pltpu.SemaphoreType.DMA] * 2,
            name="land",
        )(*map(near, pair), *outs)
    next_inputs, next_grads = outs
    return (next_inputs[None, None], next_grads[None, None], grad_down[None], grad_up[None])


def solution(mesh):
    rows = P("section", "dp", None, "tensor")
    maps = P("section", None, "tensor")
    return jax.shard_map(
        shards,
        mesh=mesh,
        in_specs=(rows, rows, rows, P("section", "dp", None), P("section", "tensor"), maps, maps),
        out_specs=(rows, rows, P("section", "dp", "tensor"), P("section", "dp", "tensor")),
        check_vma=False,
    )
```

```python
import functools

import jax
import jax.numpy as jnp
from jax import lax
from jax.experimental import pallas as pl
from jax.experimental.pallas import tpu as pltpu
from jax.sharding import PartitionSpec as P

EPSILON = 1e-05
LANES = 128
BLOCK = 512
CHUNKS = 1
KERNEL_VMEM = 32 * 1024 * 1024
F32 = jnp.float32
BF16 = jnp.bfloat16


def round_up(value, unit):
    return -(-value // unit) * unit


def partner(index, step, count):
    if count & (count - 1) == 0:
        return index ^ step
    return (index + step) % count


def source(index, step, count):
    if count & (count - 1) == 0:
        return index ^ step
    return (index - step + count) % count


def send_step(cells, axis, step):
    count = lax.axis_size(axis)
    return lax.ppermute(cells, axis, [(i, partner(i, step, count)) for i in range(count)])


def near(cells):
    return pltpu.with_memory_space_constraint(cells, pltpu.VMEM)


def contract_last(left_side, right_side):
    return lax.dot_general(left_side, right_side, (((1,), (1,)), ((), ())), preferred_element_type=F32)


def contract_rows(left_side, right_side):
    return lax.dot_general(left_side, right_side, (((0,), (0,)), ((), ())), preferred_element_type=F32)


def split_pair(values):
    high = values.astype(BF16).astype(F32)
    return high, values - high


def place_pair(slot, unit_count, pair):
    lane = lax.broadcasted_iota(jnp.int32, slot.shape, 1)
    high, low = pair
    rest = jnp.where(lane == unit_count, high, jnp.where(lane == unit_count + 1, low, 0.0))
    return jnp.where(lane < unit_count, slot, rest)


def take_pair(slot, unit_count):
    return slot[:, unit_count : unit_count + 1] + slot[:, unit_count + 1 : unit_count + 2]


def keep_mask(first_row, shape, seq_rows, lengths_ref):
    row = first_row + lax.broadcasted_iota(jnp.int32, shape, 0)
    limit = jnp.where(row < seq_rows, lengths_ref[0], lengths_ref[1] + seq_rows)
    return row < limit


def partials_body(unit_count, slot, share_count, fwd_ref, saved_ref, grad_ref, gain_ref, down_ref, up_ref, *refs):
    outs = refs[:share_count]
    acc_ref, squares_ref = refs[share_count:]
    step = pl.program_id(0)

    @pl.when(step == 0)
    def _():
        acc_ref[...] = jnp.zeros_like(acc_ref)
        squares_ref[...] = jnp.zeros_like(squares_ref)

    down = (down_ref[...].astype(F32) * gain_ref[...].astype(F32)).astype(BF16)
    for which, rows_ref in enumerate((fwd_ref, saved_ref)):
        values = rows_ref[...].astype(F32)
        lo = which * slot
        acc_ref[:, lo : lo + unit_count] += contract_last(rows_ref[...], down)
        total = squares_ref[which]
        for c in range(0, values.shape[1], LANES):
            part = values[:, c : c + LANES]
            total += part * part
        squares_ref[which] = total
    acc_ref[:, 2 * slot : 2 * slot + unit_count] += contract_last(grad_ref[...], up_ref[...])

    @pl.when(step == pl.num_programs(0) - 1)
    def _():
        for which in range(2):
            total = jnp.sum(squares_ref[which], axis=1, keepdims=True)
            lo = which * slot
            acc_ref[:, lo : lo + slot] = place_pair(acc_ref[:, lo : lo + slot], unit_count, split_pair(total))
        share_rows = outs[0].shape[0]
        for k, out in enumerate(outs):
            first = pl.multiple_of(partner(lax.axis_index("tensor"), k, share_count) * share_rows, share_rows)
            out[...] = acc_ref[pl.ds(first, share_rows), :].astype(BF16)


def middle_body(unit_count, slot, full_width, seq_rows, lengths_ref, *refs):
    parts, out = refs[:-1], refs[-1]
    total = parts[0][...].astype(F32)
    for part in parts[1:]:
        total += part[...].astype(F32)
    share_rows = total.shape[0]
    keep = keep_mask(lax.axis_index("tensor") * share_rows, (share_rows, slot), seq_rows, lengths_ref)
    fwd, saved, slope = (total[:, i * slot : (i + 1) * slot] for i in range(3))
    fwd_scale = lax.rsqrt(take_pair(fwd, unit_count) / full_width + EPSILON)
    saved_scale = lax.rsqrt(take_pair(saved, unit_count) / full_width + EPSILON)
    lane = lax.broadcasted_iota(jnp.int32, fwd.shape, 1)
    unit = lane < unit_count
    fwd_rank = fwd * fwd_scale
    saved_rank = saved * saved_scale
    gate = jax.nn.sigmoid(saved_rank)
    back = jnp.where(unit & keep, slope * (gate * (1.0 + saved_rank * (1.0 - gate))), 0.0)
    bend = saved_scale * saved_scale * (jnp.sum(back * saved_rank, axis=1, keepdims=True) / full_width)
    out[:, 0:slot] = jnp.where(unit, fwd_rank * jax.nn.sigmoid(fwd_rank), 0.0).astype(BF16)
    out[:, slot : 2 * slot] = jnp.where(unit & keep, saved_rank * gate, 0.0).astype(BF16)
    out[:, 2 * slot :] = place_pair(back * saved_scale, unit_count, split_pair(bend)).astype(BF16)


def join_shares(shares, whole_ref):
    share_rows = shares[0].shape[0]
    for k, share in enumerate(shares):
        first = source(lax.axis_index("tensor"), k, len(shares)) * share_rows
        whole_ref[pl.ds(pl.multiple_of(first, share_rows), share_rows), :] = share[...]


def edges_body(unit_count, slot, share_count, seq_rows, lengths_ref, *refs):
    shares = refs[:share_count]
    fwd_ref, saved_ref, grad_ref, gain_ref, down_ref, up_ref, out_fwd, out_grad, whole_ref = refs[share_count:]

    @pl.when(pl.program_id(0) == 0)
    def _():
        join_shares(shares, whole_ref)

    block = grad_ref.shape[1]
    here = pl.ds(pl.multiple_of(pl.program_id(0) * block, block), block)
    keep = keep_mask(0, grad_ref.shape, seq_rows, lengths_ref)
    back = whole_ref[:, 2 * slot : 2 * slot + unit_count]
    bend = take_pair(whole_ref[:, 2 * slot :].astype(F32), unit_count)
    weighted = jnp.dot(back, down_ref[...], preferred_element_type=F32) * gain_ref[...].astype(F32)
    kept = jnp.where(keep, grad_ref[...].astype(F32), 0.0)
    out_grad[:, here] = (kept + weighted - saved_ref[...].astype(F32) * bend).astype(BF16)
    act = whole_ref[:, 0:unit_count]
    lifted = jnp.dot(act, up_ref[...], preferred_element_type=F32)
    out_fwd[:, here] = (fwd_ref[...].astype(F32) + lifted).astype(BF16)


def grads_body(unit_count, slot, share_count, *refs):
    shares = refs[:share_count]
    saved_ref, grad_ref, gain_ref = refs[share_count : share_count + 3]
    outs = refs[share_count + 3 : -2]
    whole_ref, hold_ref = refs[-2:]

    @pl.when(pl.program_id(0) == 0)
    def _():
        join_shares(shares, whole_ref)

    back = whole_ref[:, 2 * slot : 2 * slot + unit_count]
    act = whole_ref[:, slot : slot + unit_count]
    hold_ref[0] = contract_rows(back, saved_ref[...]) * gain_ref[...].astype(F32)
    hold_ref[1] = contract_rows(act, grad_ref[...])
    group_count = len(outs)
    group_rows = unit_count // group_count
    block = grad_ref.shape[1]
    here = pl.ds(pl.multiple_of(pl.program_id(0) * block, block), block)
    for k, out in enumerate(outs):
        first = partner(lax.axis_index("dp"), k, group_count) * group_rows
        for which in range(2):
            out[which, :, here] = hold_ref[which, pl.ds(pl.multiple_of(first, group_rows), group_rows), :].astype(BF16)


def mean_body(*refs):
    shares, outs = refs[:-2], refs[-2:]
    block = outs[0].shape[1]
    here = pl.ds(pl.multiple_of(pl.program_id(0) * block, block), block)
    for which, out in enumerate(outs):
        total = shares[0][which, :, here].astype(F32)
        for share in shares[1:]:
            total += share[which, :, here].astype(F32)
        out[...] = (total * (1.0 / len(shares))).astype(BF16)


def land_body(first_col, span, first_ref, second_ref, *refs):
    first_out, second_out, first_sem, second_sem = refs[-4:]
    here = pl.ds(first_col, span)
    first = pltpu.make_async_copy(first_ref, first_out.at[:, here], first_sem)
    second = pltpu.make_async_copy(second_ref, second_out.at[:, here], second_sem)
    first.start()
    second.start()
    first.wait()
    second.wait()


def shards(forward_rows, saved_rows, output_grad, lengths, norm_gain, down_map, up_map):
    fwd, saved, grad = forward_rows[0, 0], saved_rows[0, 0], output_grad[0, 0]
    seq_lengths = lengths[0, 0]
    down, up = down_map[0], up_map[0]
    row_count, width = fwd.shape
    unit_count = down.shape[0]
    share_count = lax.axis_size("tensor")
    group_count = lax.axis_size("dp")
    section_count = lax.axis_size("section")
    share_rows = row_count // share_count
    seq_rows = row_count // 2
    full_width = width * share_count
    slot = round_up(unit_count + 2, LANES)
    packed = 3 * slot
    block = min(width, BLOCK)
    steps = width // block
    smem = pl.BlockSpec(memory_space=pltpu.SMEM)
    cols = lambda n: pl.BlockSpec((n, block), lambda j: (0, j))
    whole = pl.BlockSpec(memory_space=pltpu.VMEM)
    share_type = pltpu.VMEM((share_rows, packed), BF16)

    parts = pl.pallas_call(
        functools.partial(partials_body, unit_count, slot, share_count),
        grid=(steps,),
        in_specs=[cols(row_count), cols(row_count), cols(row_count), cols(1), cols(unit_count), cols(unit_count)],
        out_specs=[whole] * share_count,
        out_shape=[share_type] * share_count,
        scratch_shapes=[pltpu.VMEM((row_count, packed), F32), pltpu.VMEM((2, row_count, LANES), F32)],
        name="partials",
    )(fwd, saved, grad, norm_gain, down, up)
    got = [near(send_step(parts[k], "tensor", k)) for k in range(share_count - 1, 0, -1)] + [near(parts[0])]
    mine = pl.pallas_call(
        functools.partial(middle_body, unit_count, slot, full_width, seq_rows),
        in_specs=[smem] + [pl.BlockSpec(memory_space=pltpu.VMEM)] * share_count,
        out_specs=pl.BlockSpec(memory_space=pltpu.VMEM),
        out_shape=share_type,
        compiler_params=pltpu.CompilerParams(vmem_limit_bytes=KERNEL_VMEM),
        name="middle",
    )(seq_lengths, *got)
    shares = [near(mine)] + [near(send_step(mine, "tensor", k)) for k in range(1, share_count)]
    span = width // CHUNKS
    chunk_steps = span // block
    landed = []
    for c in range(CHUNKS):
        part = lambda n, first=c * chunk_steps: pl.BlockSpec((n, block), lambda j: (0, j + first))
        edge_rows = pl.pallas_call(
            functools.partial(edges_body, unit_count, slot, share_count, seq_rows),
            grid=(chunk_steps,),
            in_specs=[smem] + [whole] * share_count
            + [part(row_count), part(row_count), part(row_count), part(1), part(unit_count), part(unit_count)],
            out_specs=[whole] * 2,
            out_shape=[pltpu.VMEM((row_count, span), BF16)] * 2,
            scratch_shapes=[pltpu.VMEM((row_count, packed), BF16)],
            cost_estimate=pl.CostEstimate(flops=40 * row_count * unit_count * span, bytes_accessed=8 * row_count * span, transcendentals=0),
            compiler_params=pltpu.CompilerParams(vmem_limit_bytes=KERNEL_VMEM),
            name="edges",
        )
        out_fwd, out_grad = edge_rows(seq_lengths, *shares, fwd, saved, grad, norm_gain, down, up)
        next_grads = lax.ppermute(near(out_grad), "section", [(i + 1, i) for i in range(section_count - 1)])
        next_inputs = lax.ppermute(near(out_fwd), "section", [(i, i + 1) for i in range(section_count - 1)])
        landed.append((next_inputs, next_grads))
    group_rows = unit_count // group_count
    sum_maps = pl.pallas_call(
        functools.partial(grads_body, unit_count, slot, share_count),
        grid=(steps,),
        in_specs=[whole] * share_count + [cols(row_count), cols(row_count), cols(1)],
        out_specs=[whole] * group_count,
        out_shape=[pltpu.VMEM((2, group_rows, width), BF16)] * group_count,
        scratch_shapes=[pltpu.VMEM((row_count, packed), BF16), pltpu.VMEM((2, unit_count, block), F32)],
        cost_estimate=pl.CostEstimate(flops=40 * row_count * unit_count * width, bytes_accessed=6 * row_count * width, transcendentals=0),
        compiler_params=pltpu.CompilerParams(vmem_limit_bytes=KERNEL_VMEM),
        name="grads",
    )
    halves = sum_maps(*shares, saved, grad, norm_gain)
    sums = [near(halves[0])] + [near(send_step(near(halves[k]), "dp", k)) for k in range(1, group_count)]
    mean_maps = pl.pallas_call(
        mean_body,
        grid=(steps,),
        in_specs=[whole] * group_count,
        out_specs=[cols(group_rows)] * 2,
        out_shape=[jax.ShapeDtypeStruct((group_rows, width), BF16)] * 2,
        compiler_params=pltpu.CompilerParams(vmem_limit_bytes=KERNEL_VMEM),
        name="means",
    )
    grad_down, grad_up = mean_maps(*sums)
    outs = []
    for c, pair in enumerate(landed):
        outs = pl.pallas_call(
            functools.partial(land_body, c * span, span),
            in_specs=[whole] * 2 + [pl.BlockSpec(memory_space=pl.ANY)] * len(outs),
            out_specs=[pl.BlockSpec(memory_space=pl.ANY)] * 2,
            out_shape=[jax.ShapeDtypeStruct((row_count, width), BF16)] * 2,
            input_output_aliases={2: 0, 3: 1} if outs else {},
            scratch_shapes=[pltpu.SemaphoreType.DMA] * 2,
            compiler_params=pltpu.CompilerParams(vmem_limit_bytes=KERNEL_VMEM),
            name="land",
        )(*map(near, pair), *outs)
    next_inputs, next_grads = outs
    return (next_inputs[None, None], next_grads[None, None], grad_down[None], grad_up[None])


def solution(mesh):
    rows = P("section", "dp", None, "tensor")
    maps = P("section", None, "tensor")
    return jax.shard_map(
        shards,
        mesh=mesh,
        in_specs=(rows, rows, rows, P("section", "dp", None), P("section", "tensor"), maps, maps),
        out_specs=(rows, rows, P("section", "dp", "tensor"), P("section", "dp", "tensor")),
        check_vma=False,
    )
```
